32 devices in a mesh: groups: 2 (over y), seq: 8 (over z, core), side: 1, req: 2 (over x).
Axes of the slice: x: 2, y: 2, z: 4, core: 2. Of those that a mesh axis runs over, the one named last changes fastest.
Arguments:
- queries: bfloat16 [4, 128, 4, 2048], P(('groups', 'req'), 'seq', 'side'), parts along dimension 0, may hold values from -8 to 8
- cache_keys: bfloat16 [4, 1024, 512], P(('groups', 'req'), 'seq', 'side'), parts along dimension 0, may hold values from -8 to 8
- cache_values: bfloat16 [4, 1024, 512], P(('groups', 'req'), 'seq', 'side'), parts along dimension 0, may hold values from -6 to 6
- tree_keys: bfloat16 [4, 128, 512], P(('groups', 'req'), 'seq', 'side'), parts along dimension 0, may hold values from -8 to 8
- tree_values: bfloat16 [4, 128, 512], P(('groups', 'req'), 'seq', 'side'), parts along dimension 0, may hold values from -6 to 6
- parents: int32 [4, 128], P(('groups', 'req')), parts along dimension 0, may hold values from 0 to 126, as said below
- lengths: int32 [4], P(('groups', 'req')), parts along dimension 0, may hold values from 128 to 1024
- out_weight: bfloat16 [4, 2048, 4096], P('side', 'seq', 'req'), may hold values from -0.0625 to 0.0625
- in_experts: bfloat16 [64, 4096, 1024], P(('seq', 'side'), 'req'), may hold values from -0.09375 to 0.09375
- out_experts: bfloat16 [64, 1024, 4096], P(('seq', 'side'), None, 'req'), may hold values from -0.1875 to 0.1875
- gate_experts: int32 [512, 8], P(('groups', 'seq', 'side')), parts along dimension 0, may hold values from 0 to 63, all different within a row; in each aligned block of 32 rows (0 to 31, 32 to 63, ...) at most 6 rows name the same one
- gate_weights: float32 [512, 8], P(('groups', 'seq', 'side')), parts along dimension 0, may hold values from 0.1 to 1
Outputs:
- attended: bfloat16 [512, 4096], P(('groups', 'seq', 'side'), 'req'), parts along dimension 0
- expert_out: bfloat16 [512, 4096], P(('groups', 'seq', 'side'), 'req'), parts along dimension 0
The draws below stay inside these ranges and needn't reach their ends.
There are 2 independent parts, one for each index of `groups`. The reference program is written for one: setup_inputs(seed, part) draws one part's arguments, and reference() takes and returns one part's arrays. A program takes and returns all parts, laid end to end along the dimension named above; an argument that names none is the same for every part. Nothing has to cross between parts.
Inputs may be any that keep to these rules, and one draw needn't show every extreme that they name: parents[r, 0] is 0; every node i >= 1 has its parent among nodes i - 4 to i - 1. `gate_experts`: within the 32 rows that one device holds along seq+side, no expert is named by more than 6 rows, and in some such block one expert is named exactly 6 times.
All inputs are finite; a program needn't handle non-finite values.
Results may differ from the reference program's by a relative error of at most 0.018.
Values may be sent and summed in bfloat16 or wider, within the bound.
No kernel may reach another device: no remote copies, remote signals or barrier semaphores. Data moves between devices by JAX's collectives and lax.ppermute only.
A program may use at most 128 MiB of HBM per device.

```python
import math
import jax
import jax.numpy as jnp
import numpy as np
from jax import lax

D = 4096
KVH = 4
GROUP = 16
HD = 128
EXPERTS = 64
FF_E = 1024
TOP = 8
CAP = 6
NODES = 128
CTX = 1024
REQS = 2
TOKENS = 256
TOK_MOE = 32


def draw_queries(key, part):
    shape_all = (REQS, NODES, KVH, GROUP * HD)
    drawn = jnp.clip(1.7 * jax.random.normal(jax.random.fold_in(key, 12), shape_all, jnp.float32), -8.0, 8.0)
    return drawn.astype(jnp.bfloat16)


def draw_cache_keys(key, part):
    shape_all = (REQS, CTX, KVH * HD)
    drawn = jnp.clip(1.7 * jax.random.normal(jax.random.fold_in(key, 22), shape_all, jnp.float32), -8.0, 8.0)
    return drawn.astype(jnp.bfloat16)


def draw_parents(key, part):
    backward = jax.random.randint(jax.random.fold_in(key, 31), (REQS, NODES), 1, 5)
    node_ids = jnp.arange(NODES, dtype=jnp.int32)[None, :]
    return (node_ids - jnp.minimum(backward, node_ids)).astype(jnp.int32)


def block_levels(key, shape, shards, smallest, largest):
    def one(position, blocks):
        steps = jax.random.uniform(jax.random.fold_in(jax.random.fold_in(key, 6), position), (blocks,), jnp.float32, smallest / len(shards), largest / len(shards))
        return jnp.repeat(jnp.exp(steps), shape[position] // blocks).reshape((-1,) + (1,) * (len(shape) - position - 1))

    loudness = one(*shards[0])
    for cut in shards[1:]:
        loudness = loudness * one(*cut)
    return loudness


def routed_block(rng, own, number, rows, number_of, top, bound, skew):
    order = jax.random.permutation(rng, number_of)
    heavy_load, usual = shares(number_of, rows * top, bound, skew, True), shares(number_of, rows * top, bound, skew, False)
    places = jnp.arange(number_of)

    def named(tallies, rotation):
        used = int((tallies > 0).sum())
        fixed = max(1, used // 4)
        shifted = fixed + (places - fixed + rotation * (used - fixed)) % max(1, number_of - fixed)
        return jnp.zeros((number_of,), jnp.int32).at[order[jnp.where(places < fixed, places, shifted)]].set(jnp.asarray(tallies, jnp.int32))

    tallies = jnp.where(number % 4 == 0, named(heavy_load, number // 4), named(usual, number - number // 4 - 1))
    mixed = jax.random.permutation(jax.random.fold_in(own, 3), number_of)
    giver, receiver = mixed[0:number_of // 2 * 2:2], mixed[1:number_of // 2 * 2:2]
    room = jnp.minimum(tallies[giver] - 1, bound - tallies[receiver]) // 2
    room = jnp.where((giver == order[0]) | (receiver == order[0]) | (tallies[receiver] == 0), 0, jnp.maximum(room, 0))
    shifted = jax.random.randint(jax.random.fold_in(own, 4), (number_of // 2,), 0, 1 << 20) % (room + 1)
    tallies = tallies.at[giver].add(-shifted).at[receiver].add(shifted)
    items = jnp.searchsorted(jnp.cumsum(tallies), jnp.arange(rows * top), side="right").astype(jnp.int32)
    listing = items.reshape(top, rows).T
    listing = listing[jax.random.permutation(jax.random.fold_in(own, 1), rows)]
    rotation = jax.random.randint(jax.random.fold_in(own, 2), (rows, 1), 0, top)
    return jnp.take_along_axis(listing, (jnp.arange(top)[None, :] + rotation) % top, axis=1)


def shares(number_of, total, reach, slope, full):
    loads = [(1 << 20) // math.isqrt(grade ** slope) + 1 for grade in range(1, number_of + 1)]
    largest = reach if full else min(reach, max(-(-total // number_of), total * loads[0] // sum(loads)))
    least = 1 if total - largest >= number_of - 1 else 0
    given, surplus = [largest] + [least] * (number_of - 1), total - largest - least * (number_of - 1)
    while surplus > 0:
        movable = [i for i in range(1, number_of) if given[i] < largest] or [i for i in range(1, number_of) if given[i] < reach]
        whole, left = sum([loads[i] for i in movable]), surplus
        for i in movable:
            more = min(reach - given[i], max(1, left * loads[i] // whole), surplus)
            given[i] = given[i] + more
            surplus = surplus - more
    return np.array(given)


def scatter_about(own_key, dims, spread, reach, shards=(), kind=jnp.bfloat16):
    values = jax.random.normal(own_key, dims, jnp.float32) * spread
    if len(shards) > 0:
        values = block_levels(own_key, dims, shards, -0.22, 0.18) * values
    return jnp.clip(values, min=-reach, max=reach).astype(kind)


def setup_inputs(seed: int = 0, part: int = 0) -> dict:
    streams_of = jax.random.split(jax.random.key(seed), 13)
    part_splits = jax.random.split(jax.random.fold_in(streams_of[12], part), 13)
    queries = draw_queries(jax.random.fold_in(jax.random.fold_in(streams_of[12], part), 71), part)
    cache_keys = draw_cache_keys(jax.random.fold_in(jax.random.fold_in(streams_of[12], part), 71), part)
    cache_values = scatter_about(part_splits[2], (REQS, CTX, KVH * HD), 1.0, 6.0, ((0, 2), (1, 8)))
    tree_keys = scatter_about(part_splits[3], (REQS, NODES, KVH * HD), 1.7, 8.0, ((0, 2), (1, 8)))
    tree_values = scatter_about(part_splits[4], (REQS, NODES, KVH * HD), 1.0, 6.0, ((0, 2), (1, 8)))
    parents = draw_parents(jax.random.fold_in(jax.random.fold_in(streams_of[12], part), 71), part)
    lengths = jax.random.randint(part_splits[6], (REQS,), CTX // 8, CTX + 1).astype(jnp.int32)
    out_weight = scatter_about(streams_of[7], (KVH, GROUP * HD, D), (KVH * GROUP * HD) ** -0.5, 0.0625, ((1, 8), (2, 2)))
    in_experts = scatter_about(streams_of[8], (EXPERTS, D, FF_E), D ** -0.5, 0.09375, ((0, 8), (1, 2)))
    out_experts = scatter_about(streams_of[9], (EXPERTS, FF_E, D), FF_E ** -0.5, 0.1875, ((0, 8), (2, 2)))
    gate_experts_keys = jax.random.split(jax.random.fold_in(part_splits[10], 1), TOKENS // TOK_MOE)
    gate_experts_turns = jax.random.permutation(jax.random.fold_in(part_splits[10], 3), TOKENS // TOK_MOE)
    gate_experts = jax.vmap(lambda own, number: routed_block(jax.random.fold_in(part_splits[10], 2), own, number, TOK_MOE, EXPERTS, TOP, CAP, 2))(gate_experts_keys, gate_experts_turns).reshape((TOKENS, TOP))
    gate_weights = jnp.clip(jnp.exp(math.log(1.0) - 2.3025851 * jax.random.uniform(part_splits[11], (TOKENS, TOP), jnp.float32) ** block_levels(part_splits[11], (TOKENS, TOP), ((0, 8),), -0.2, 0.2)), 0.1, 1.0)
    return {"queries": queries, "cache_keys": cache_keys, "cache_values": cache_values, "tree_keys": tree_keys, "tree_values": tree_values, "parents": parents, "lengths": lengths, "out_weight": out_weight, "in_experts": in_experts, "out_experts": out_experts, "gate_experts": gate_experts, "gate_weights": gate_weights}


def ancestors(parent_row):
    node_ids = jnp.arange(NODES, dtype=jnp.int32)
    parent_hit = (node_ids[None, :] == parent_row[:, None]).astype(jnp.float32)
    reached = jnp.maximum(parent_hit, jnp.eye(NODES, dtype=jnp.float32))
    for turn_number in range(max(1, (NODES - 1).bit_length())):
        reached = jnp.minimum(jnp.dot(reached, reached, precision=lax.Precision.HIGHEST), 1.0)
    return reached

def attend_request(operands):
    query_all, key_cache, value_cache, key_tree, value_tree, parent_row, length = operands
    reached = ancestors(parent_row)
    context_seen = jnp.arange(CTX, dtype=jnp.int32) < length
    visible = jnp.concatenate([jnp.broadcast_to(context_seen[None, :], (NODES, CTX)), reached > 0.5], axis=1)
    factor = 1.0 / math.sqrt(HD)
    results = []
    for head_pair in range(KVH):
        first_col = head_pair * HD
        key_rows = jnp.concatenate([key_cache[:, first_col:first_col + HD], key_tree[:, first_col:first_col + HD]], axis=0).astype(jnp.float32)
        value_rows = jnp.concatenate([value_cache[:, first_col:first_col + HD], value_tree[:, first_col:first_col + HD]], axis=0).astype(jnp.float32)
        query_block = query_all[:, head_pair].reshape(NODES, GROUP, HD).astype(jnp.float32)
        scores = jnp.einsum('ngd,kd->ngk', query_block, key_rows, precision=lax.Precision.HIGHEST) * factor
        scores = jnp.where(visible[:, None, :], scores, -jnp.inf)
        weights = jax.nn.softmax(scores, axis=-1)
        weights_low = lax.optimization_barrier(weights.astype(jnp.bfloat16)).astype(jnp.float32)
        results.append(jnp.einsum('ngk,kd->ngd', weights_low, value_rows, precision=lax.Precision.HIGHEST))
    return jnp.stack(results, axis=1)

def reference(queries, cache_keys, cache_values, tree_keys, tree_values, parents, lengths, out_weight, in_experts, out_experts, gate_experts, gate_weights):
    attention = lax.map(attend_request, (queries, cache_keys, cache_values, tree_keys, tree_values, parents, lengths))
    attention = attention.reshape(REQS * NODES, KVH * GROUP * HD).astype(jnp.bfloat16)
    projector = out_weight.reshape(KVH * GROUP * HD, D).astype(jnp.float32)
    attended = jnp.dot(attention.astype(jnp.float32), projector, precision=lax.Precision.HIGHEST).astype(jnp.bfloat16)
    token_count = REQS * NODES
    limit = token_count // TOK_MOE * CAP
    token_ids = jnp.arange(token_count, dtype=jnp.int32)

    def add_expert(carry, expert_id):
        chosen = gate_experts == expert_id
        coefficient = lax.optimization_barrier(jnp.sum(jnp.where(chosen, gate_weights, 0.0), axis=1))
        user = jnp.any(chosen, axis=1)
        order = jnp.argsort(jnp.where(user, 0, 1).astype(jnp.int32) * token_count + token_ids)[:limit].astype(jnp.int32)
        row_block = attended[order].astype(jnp.float32)
        before = jnp.dot(row_block, in_experts[expert_id].astype(jnp.float32), precision=lax.Precision.HIGHEST)
        hidden = jax.nn.silu(before).astype(jnp.bfloat16)
        produced = jnp.dot(hidden.astype(jnp.float32), out_experts[expert_id].astype(jnp.float32), precision=lax.Precision.HIGHEST).astype(jnp.bfloat16)
        produced = lax.optimization_barrier(produced).astype(jnp.float32)
        return (carry.at[order].add(coefficient[order][:, None] * produced), None)
    summed, unused_rows = lax.scan(add_expert, jnp.zeros((token_count, D), jnp.float32), jnp.arange(EXPERTS, dtype=jnp.int32))
    return (attended, summed.astype(jnp.bfloat16))
```

```python
import math

import jax
import jax.numpy as jnp
from jax import lax
from jax.experimental import pallas as pl
from jax.experimental.pallas import tpu as pltpu
from jax.sharding import PartitionSpec as P

GROUP = 16
HD = 128
EXPERTS = 64
CAP = 6
NEG_FILL = -1e30
F32 = jnp.float32
BF16 = jnp.bfloat16


def call(body, outs, n_in, scratch=(), vmem=48 << 20, flops=1_000_000):
    return pl.pallas_call(
        body,
        out_shape=outs,
        in_specs=[pl.BlockSpec(memory_space=pltpu.SMEM)]
        + [pl.BlockSpec(memory_space=pltpu.VMEM)] * n_in,
        out_specs=jax.tree.map(lambda _: pl.BlockSpec(memory_space=pltpu.VMEM), outs),
        scratch_shapes=list(scratch),
        compiler_params=pltpu.CompilerParams(vmem_limit_bytes=vmem),
        cost_estimate=pl.CostEstimate(flops=flops, transcendentals=0, bytes_accessed=1_000_000),
    )


def shape(dims, kind=BF16):
    return jax.ShapeDtypeStruct(dims, kind)


def dot(a, b, dims=((1,), (0,))):
    return lax.dot_general(a, b, (dims, ((), ())), preferred_element_type=F32)


def pack_blocks(scalars, chips, cached, tree, nodes, group_cols, keys, tkeys, values, tvalues, mine, other, route):
    kv_rows = cached + tree
    q_rows = 2 * nodes
    rows = kv_rows + chips * q_rows + route.shape[0]

    def body(s_ref, k_ref, tk_ref, v_ref, tv_ref, m_ref, o_ref, r_ref, *outs):
        z = s_ref[0]
        for k in range(chips):
            zk = z ^ k
            cols = pl.ds(pl.multiple_of(zk * HD, HD), HD)
            out = outs[k]
            out[:cached, :HD] = k_ref[:, cols]
            out[cached:kv_rows, :HD] = tk_ref[:, cols]
            out[:cached, HD:] = v_ref[:, cols]
            out[cached:kv_rows, HD:] = tv_ref[:, cols]
            for target in range(chips):
                at = kv_rows + target * q_rows
                out[at : at + nodes] = m_ref[zk, target]
                out[at + nodes : at + q_rows] = o_ref[zk, target]
            out[rows - route.shape[0] :] = r_ref[...]

    return call(body, [shape((rows, group_cols))] * chips, 7)(
        scalars, keys, tkeys, values, tvalues, mine, other, route
    )


def visibility(scalars, chips, cached, tree, parent_row):
    total = 2 * chips * tree
    ctx = 2 * chips * cached
    turns = max(1, (total - 1).bit_length())

    def body(s_ref, p_ref, out):
        z, c, length = s_ref[0], s_ref[1], s_ref[2]
        rows = lax.broadcasted_iota(jnp.int32, (total, total), 0)
        cols = lax.broadcasted_iota(jnp.int32, (total, total), 1)
        hit = (jnp.broadcast_to(p_ref[...], (total, total)) == rows) | (rows == cols)
        reach = hit.astype(F32).astype(BF16)
        for _ in range(turns):
            reach = jnp.minimum(dot(reach, reach), 1.0).astype(BF16)
        block = rows // tree
        node = (((z ^ (block >> 1)) << 1) | (c ^ (block & 1))) * tree + rows % tree
        order = (node == cols).astype(F32).astype(BF16)
        left = dot(order, reach, ((1,), (1,))).astype(BF16)
        seen = dot(left, order, ((1,), (1,)))
        out[:, ctx:] = jnp.where(seen > 0.5, 0.0, NEG_FILL)
        lane = lax.broadcasted_iota(jnp.int32, (total, ctx), 1)
        block = lane // cached
        place = (((z ^ (block >> 1)) << 1) | (c ^ (block & 1))) * cached + lane % cached
        out[:, :ctx] = jnp.where(place < length, 0.0, NEG_FILL)

    return call(body, shape((total, ctx + total), F32), 1, flops=40_000_000)(scalars, parent_row)


def attend(scalars, chips, cached, tree, own, partner, bias):
    total, width = bias.shape
    ctx = 2 * chips * cached
    kv_rows = cached + tree
    q_rows = total // chips
    per = own[0].shape[1] // HD
    factor = 1.0 / math.sqrt(HD)

    def body(s_ref, *refs):
        blocks = (refs[:chips], refs[chips : 2 * chips])
        b_ref = refs[2 * chips]
        outs = refs[2 * chips + 1 : 3 * chips + 1]
        keys, values, rows = refs[3 * chips + 1 :]
        z, c = s_ref[0], s_ref[1]
        for k in range(chips):
            for t in range(2):
                b, src = 2 * k + t, blocks[t][k]
                for dst, cols in ((keys, slice(0, HD)), (values, slice(HD, 2 * HD))):
                    dst[b * cached : (b + 1) * cached] = src[:cached, cols]
                    dst[ctx + b * tree : ctx + (b + 1) * tree] = src[cached:kv_rows, cols]
        for kk in range(chips):
            at = pl.ds(pl.multiple_of(kv_rows + (z ^ kk) * q_rows, 16), q_rows)
            for j in range(per):
                for k in range(chips):
                    first = j * total + k * q_rows
                    rows[first : first + q_rows] = blocks[0][k][at, j * HD : (j + 1) * HD]
            scores = dot(rows[...], keys[...], ((1,), (1,))) * factor
            scores = (scores.reshape(per, total, width) + b_ref[...][None]).reshape(per * total, width)
            top = jnp.max(scores, axis=-1, keepdims=True)
            weights = jnp.exp(scores - top)
            mass = jnp.sum(weights, axis=-1, keepdims=True)
            result = (dot(weights.astype(BF16), values[...]) / mass).astype(BF16)
            for j in range(per):
                for k in range(chips):
                    for t in range(2):
                        first = j * total + k * q_rows + t * tree
                        node = pl.multiple_of((((z ^ k) << 1) | (c ^ t)) * tree, 16)
                        outs[kk][pl.ds(node, tree), j * HD : (j + 1) * HD] = result[first : first + tree]

    return call(
        body,
        [shape((total, per * HD))] * chips,
        2 * chips + 1,
        [pltpu.VMEM((width, HD), BF16), pltpu.VMEM((width, HD), BF16), pltpu.VMEM((per * total, HD), BF16)],
        flops=4 * per * chips * total * width * HD,
    )(scalars, *own, *partner, bias)


def project(scalars, chips, own, other, weight, tile=512):
    rows, depth = own[0].shape
    cols = weight.shape[2]
    block = 2 * rows // (2 * chips)

    def body(s_ref, *refs):
        w_ref, mine, theirs = refs[2 * chips], refs[2 * chips + 1], refs[2 * chips + 2]
        z, c, x = s_ref[0], s_ref[1], s_ref[3]
        for r in range(2):
            total = None
            for k in range(chips):
                part = dot(refs[r * chips + k][...], w_ref[z ^ k])
                total = part if total is None else total + part
            for b in range(rows // block):
                k = z ^ ((x ^ r) * (chips // 2) + b // 2)
                piece = total[b * block : (b + 1) * block]

                @pl.when(c == b % 2)
                def _():
                    mine[k] = piece

                @pl.when(c != b % 2)
                def _():
                    theirs[k] = piece.astype(BF16)

    whole = pl.BlockSpec((rows, depth), lambda n: (0, 0))
    return pl.pallas_call(
        body,
        grid=(cols // tile,),
        out_shape=(shape((chips, block, cols), F32), shape((chips, block, cols))),
        in_specs=[pl.BlockSpec(memory_space=pltpu.SMEM)]
        + [whole] * (2 * chips)
        + [pl.BlockSpec((chips, depth, tile), lambda n: (0, 0, n))],
        out_specs=(pl.BlockSpec((chips, block, tile), lambda n: (0, 0, n)),) * 2,
        compiler_params=pltpu.CompilerParams(vmem_limit_bytes=32 << 20),
        cost_estimate=pl.CostEstimate(
            flops=4 * rows * chips * depth * cols, transcendentals=0, bytes_accessed=2 * weight.size
        ),
    )(scalars, *own, *other, weight)


def routing(scalars, chips, own, partner, local, slots, top, first_row):
    per = own[0].shape[0] - first_row
    tokens = 2 * chips * per
    count = local * slots

    def body(s_ref, *refs):
        pick, gate, table = refs[2 * chips], refs[2 * chips + 1], refs[2 * chips + 2]
        base = s_ref[4].astype(F32)
        for k in range(chips):
            for t in range(2):
                b = 2 * k + t
                table[b * per : (b + 1) * per] = refs[t * chips + k][first_row:, :HD].astype(F32)
        lane = lax.broadcasted_iota(jnp.int32, (tokens, HD), 1)
        expert = jnp.where(lane < local, base + lane.astype(F32), -1.0)
        zero = jnp.zeros((tokens, HD), F32)
        hit, high, low = zero, zero, zero
        for n in range(top):
            same = table[:, n : n + 1] == expert
            hit = jnp.where(same, 1.0, hit)
            high = jnp.where(same, table[:, top + n : top + n + 1], high)
            low = jnp.where(same, table[:, 2 * top + n : 2 * top + n + 1], low)
        earlier = lax.broadcasted_iota(jnp.int32, (tokens, tokens), 1) < lax.broadcasted_iota(
            jnp.int32, (tokens, tokens), 0
        )
        rank = dot(earlier.astype(F32).astype(BF16), hit.astype(BF16))
        row = lax.broadcasted_iota(jnp.int32, (HD, count), 0)
        col = lax.broadcasted_iota(jnp.int32, (HD, count), 1)
        spread = ((col >= row * slots) & (col < (row + 1) * slots)).astype(F32).astype(BF16)
        hit_at = dot(hit.astype(BF16), spread)
        rank_at = dot(rank.astype(BF16), spread)
        slot = (lax.broadcasted_iota(jnp.int32, (tokens, count), 1) % slots).astype(F32)
        placed = ((hit_at > 0.5) & (rank_at == slot)).astype(F32)
        placing = placed.T.astype(BF16)
        pick[...] = placing
        weights = dot(placing, high.astype(BF16)) + dot(placing, low.astype(BF16))
        mine = lax.broadcasted_iota(jnp.int32, (count, HD), 0) // slots == lax.broadcasted_iota(
            jnp.int32, (count, HD), 1
        )
        total = jnp.sum(jnp.where(mine, weights, 0.0), axis=1, keepdims=True)
        gate[...] = jnp.broadcast_to(total, (count, HD))

    return call(
        body,
        (shape((count, tokens)), shape((count, HD), F32)),
        2 * chips,
        [pltpu.VMEM((tokens, HD), F32)],
        flops=100_000_000,
    )(scalars, *own, *partner)


def expert_in(chips, own, partner, pick, weight, first, experts, slots, tile=512):
    rows, depth = own[0].shape
    tokens = 2 * chips * rows
    width = weight.shape[2]

    def body(*refs):
        p_ref, w_ref, out, table, picked = refs[2 * chips :]
        e, n = pl.program_id(0), pl.program_id(1)

        @pl.when((e == 0) & (n == 0))
        def _():
            for k in range(chips):
                for t in range(2):
                    b = 2 * k + t
                    table[b * rows : (b + 1) * rows] = refs[t * chips + k][...]

        @pl.when(n == 0)
        def _():
            picked[...] = dot(p_ref[...], table[...]).astype(BF16)

        out[...] = dot(picked[...], w_ref[0]).astype(BF16)

    block = pl.BlockSpec((rows, depth), lambda e, n: (0, 0))
    return pl.pallas_call(
        body,
        grid=(experts, width // tile),
        out_shape=shape((experts * slots, width)),
        in_specs=[block] * (2 * chips)
        + [
            pl.BlockSpec((slots, tokens), lambda e, n: (first + e, 0)),
            pl.BlockSpec((1, depth, tile), lambda e, n: (first + e, 0, n)),
        ],
        out_specs=pl.BlockSpec((slots, tile), lambda e, n: (e, n)),
        scratch_shapes=[pltpu.VMEM((tokens, depth), BF16), pltpu.VMEM((slots, depth), BF16)],
        compiler_params=pltpu.CompilerParams(vmem_limit_bytes=32 << 20),
        cost_estimate=pl.CostEstimate(
            flops=2 * experts * slots * depth * width,
            transcendentals=0,
            bytes_accessed=2 * experts * depth * width,
        ),
    )(*own, *partner, pick, weight)


def expert_out(before, before_other, gate, weight, first, experts, slots, tile=1024):
    depth, width = weight.shape[1:]

    def body(a_ref, b_ref, g_ref, w_ref, out, hidden):
        @pl.when(pl.program_id(1) == 0)
        def _():
            total = a_ref[...].astype(F32) + b_ref[...].astype(F32)
            value = total / (1.0 + jnp.exp(-total)) * g_ref[:, :1]
            hidden[...] = value.astype(BF16)

        out[...] = dot(hidden[...], w_ref[0]).astype(BF16)

    rows = pl.BlockSpec((slots, depth), lambda e, n: (e, 0))
    return pl.pallas_call(
        body,
        grid=(experts, width // tile),
        out_shape=shape((experts * slots, width)),
        in_specs=[
            rows,
            rows,
            pl.BlockSpec((slots, HD), lambda e, n: (first + e, 0)),
            pl.BlockSpec((1, depth, tile), lambda e, n: (first + e, 0, n)),
        ],
        out_specs=pl.BlockSpec((slots, tile), lambda e, n: (e, n)),
        scratch_shapes=[pltpu.VMEM((slots, depth), BF16)],
        compiler_params=pltpu.CompilerParams(vmem_limit_bytes=32 << 20),
        cost_estimate=pl.CostEstimate(
            flops=2 * experts * slots * depth * width,
            transcendentals=0,
            bytes_accessed=2 * experts * depth * width,
        ),
    )(before, before_other, gate, weight)


def combine(chips, pick, produced, tile=512):
    count, tokens = pick.shape
    chunks = len(produced)
    step, cols = produced[0].shape
    rows = tokens // (2 * chips)

    def body(p_ref, *refs):
        mine, theirs = refs[chunks:]
        total = None
        for n in range(chunks):
            part = dot(p_ref[n * step : (n + 1) * step], refs[n][...], ((0,), (0,)))
            total = part if total is None else total + part
        for k in range(chips):
            at = 2 * k * rows
            mine[k] = total[at : at + rows]
            theirs[k] = total[at + rows : at + 2 * rows].astype(BF16)

    return pl.pallas_call(
        body,
        grid=(cols // tile,),
        out_shape=(shape((chips, rows, cols), F32), shape((chips, rows, cols))),
        in_specs=[pl.BlockSpec((count, tokens), lambda n: (0, 0))]
        + [pl.BlockSpec((step, tile), lambda n: (0, n))] * chunks,
        out_specs=(pl.BlockSpec((chips, rows, tile), lambda n: (0, 0, n)),) * 2,
        compiler_params=pltpu.CompilerParams(vmem_limit_bytes=32 << 20),
        cost_estimate=pl.CostEstimate(
            flops=2 * count * tokens * cols, transcendentals=0, bytes_accessed=4 * count * cols
        ),
    )(pick, *produced)


def device_by_chips(
    chips,
    queries,
    cache_keys,
    cache_values,
    tree_keys,
    tree_values,
    parents,
    lengths,
    out_weight,
    in_experts,
    out_experts,
    gate_experts,
    gate_weights,
):
    count = 2 * chips
    index = lax.axis_index("seq")
    chip, core = index // 2, index % 2
    local = in_experts.shape[0]
    top = gate_experts.shape[1]
    slots = count * CAP
    cached, tree, nodes = cache_keys.shape[1], tree_keys.shape[1], queries.shape[1]
    heads = GROUP // count
    scalars = jnp.stack(
        [chip, core, lengths[0], lax.axis_index("req"), index * local]
    ).astype(jnp.int32)

    def to_partner(a):
        return lax.ppermute(a, "seq", [(i, i ^ 1) for i in range(count)])

    def to_chip(a, k):
        return lax.ppermute(a, "seq", [(i, i ^ (2 * k)) for i in range(count)])

    def over_req(a):
        return lax.ppermute(a, "req", [(0, 1), (1, 0)])

    def scatter_sum(mine, theirs):
        paired = mine + to_partner(theirs).astype(F32)
        sent = [to_chip(paired[k].astype(BF16), k) for k in range(1, chips)]
        total = paired[0]
        for piece in sent:
            total = total + piece.astype(F32)
        return total.astype(BF16)

    split = queries[0].reshape(nodes, chips, chips, 2, heads * HD).transpose(3, 1, 2, 0, 4)
    mine = lax.dynamic_index_in_dim(split, core, 0, keepdims=False)
    theirs = lax.dynamic_index_in_dim(split, 1 - core, 0, keepdims=False)
    high = lax.reduce_precision(gate_weights, 8, 7)
    low = gate_weights - high
    route = jnp.concatenate([gate_experts.astype(F32), high, low], axis=1)
    route = jnp.pad(route, ((0, 0), (0, heads * HD - 3 * top))).astype(BF16)
    packed = pack_blocks(
        scalars, chips, cached, tree, nodes, heads * HD,
        cache_keys[0], tree_keys[0], cache_values[0], tree_values[0], mine, to_partner(theirs), route,
    )
    own = [packed[0]] + [to_chip(packed[k], k) for k in range(1, chips)]
    partner = [to_partner(block) for block in own]
    bias = visibility(scalars, chips, cached, tree, parents)
    first_row = packed[0].shape[0] - route.shape[0]
    pick, gate = routing(scalars, chips, own, partner, local, slots, top, first_row)
    results = attend(scalars, chips, cached, tree, own, partner, bias)
    results = [results[0]] + [to_chip(results[k], k) for k in range(1, chips)]
    swapped = [over_req(block) for block in results]
    attended = scatter_sum(*project(scalars, chips, results, swapped, out_weight))
    rows = [attended] + [to_chip(attended, k) for k in range(1, chips)]
    rows_partner = [to_partner(block) for block in rows]
    step = max(1, local // 4)
    before = [
        expert_in(chips, rows, rows_partner, pick, in_experts, first, step, slots)
        for first in range(0, local, step)
    ]
    before_other = [over_req(part) for part in before]
    produced = [
        expert_out(before[n], before_other[n], gate, out_experts, n * step, step, slots)
        for n in range(len(before))
    ]
    return (attended, scatter_sum(*combine(chips, pick, produced)))


def ancestors(parent_row, node_count):
    node_ids = jnp.arange(node_count, dtype=jnp.int32)
    parent_hit = (node_ids[None, :] == parent_row[:, None]).astype(jnp.float32)
    reached = jnp.maximum(parent_hit, jnp.eye(node_count, dtype=jnp.float32))
    for turn_number in range(max(1, (node_count - 1).bit_length())):
        reached = jnp.minimum(jnp.dot(reached, reached, precision=lax.Precision.HIGHEST), 1.0)
    return reached


def per_device(
    queries,
    cache_keys,
    cache_values,
    tree_keys,
    tree_values,
    parents,
    lengths,
    out_weight,
    in_experts,
    out_experts,
    gate_experts,
    gate_weights,
):
    seq_index = lax.axis_index("seq")
    ctx_local = cache_keys.shape[1]
    nodes_local = queries.shape[1]
    kv_local = queries.shape[2]
    gathered = lax.all_gather(queries, "seq", axis=1, tiled=True)
    node_count = gathered.shape[1]
    reached = ancestors(parents[0], node_count)
    tree_seen = lax.dynamic_slice_in_dim(reached, seq_index * nodes_local, nodes_local, 1) > 0.5
    positions = seq_index * ctx_local + jnp.arange(ctx_local, dtype=jnp.int32)
    context_seen = jnp.broadcast_to((positions < lengths[0])[None, :], (node_count, ctx_local))
    visible = jnp.concatenate([context_seen, tree_seen], axis=1)[None]
    factor = 1.0 / math.sqrt(HD)
    outputs, maxima, totals = ([], [], [])
    for head_pair in range(kv_local):
        first_col = head_pair * HD
        key_rows = jnp.concatenate(
            [
                cache_keys[0, :, first_col : first_col + HD],
                tree_keys[0, :, first_col : first_col + HD],
            ],
            axis=0,
        )
        value_rows = jnp.concatenate(
            [
                cache_values[0, :, first_col : first_col + HD],
                tree_values[0, :, first_col : first_col + HD],
            ],
            axis=0,
        )
        query_block = gathered[0, :, head_pair].reshape(node_count, GROUP, HD)
        scores = (
            jnp.einsum("ngd,kd->gnk", query_block, key_rows, preferred_element_type=jnp.float32)
            * factor
        )
        masked = jnp.where(visible, scores, NEG_FILL)
        row_max = jnp.max(masked, axis=-1)
        weights = jnp.where(visible, jnp.exp(masked - row_max[..., None]), 0.0)
        weights_low = weights.astype(jnp.bfloat16)
        outputs.append(
            jnp.einsum("gnk,kd->gnd", weights_low, value_rows, preferred_element_type=jnp.float32)
        )
        maxima.append(row_max)
        totals.append(jnp.sum(weights, axis=-1))
    partial_out = jnp.stack(outputs)
    partial_max = jnp.stack(maxima)
    partial_sum = jnp.stack(totals)
    pieces = (
        lax.all_to_all(partial_out[None], "seq", split_axis=2, concat_axis=0, tiled=True),
        lax.all_to_all(partial_max[None], "seq", split_axis=2, concat_axis=0, tiled=True),
        lax.all_to_all(partial_sum[None], "seq", split_axis=2, concat_axis=0, tiled=True),
    )
    larger = jnp.max(pieces[1], axis=0)
    scales = jnp.exp(pieces[1] - larger[None])
    merged = jnp.sum(pieces[0] * scales[..., None], axis=0)
    summed = jnp.sum(pieces[2] * scales, axis=0)
    attention = merged / summed[..., None]
    attention = jnp.transpose(attention, (2, 0, 1, 3)).reshape(node_count, -1).astype(jnp.bfloat16)
    head_rows = lax.all_gather(attention, "req", axis=0, tiled=True)
    projector = out_weight.reshape(-1, out_weight.shape[2])
    attended = lax.psum_scatter(
        jnp.dot(head_rows, projector, preferred_element_type=jnp.float32),
        ("seq", "side"),
        scatter_dimension=0,
        tiled=True,
    ).astype(jnp.bfloat16)
    local_experts = in_experts.shape[0]
    flat_ids = gate_experts.reshape(-1)
    expert_hit = (flat_ids[:, None] == jnp.arange(EXPERTS, dtype=jnp.int32)[None, :]).astype(
        jnp.int32
    )
    earlier = jnp.cumsum(expert_hit, axis=0) - expert_hit
    slot_rank = jnp.sum(earlier * expert_hit, axis=1)
    slot_ids = (flat_ids * CAP + slot_rank).reshape(gate_experts.shape)
    slot_count = EXPERTS * CAP
    matches = jnp.arange(slot_count, dtype=jnp.int32)[:, None, None] == slot_ids[None]
    placing = jnp.any(matches, axis=2).astype(jnp.bfloat16)
    mixing = jnp.sum(jnp.where(matches, gate_weights[None], 0.0), axis=2)
    outgoing = jnp.dot(placing, attended, preferred_element_type=jnp.float32).astype(jnp.bfloat16)
    device_count = EXPERTS // local_experts
    outgoing = outgoing.reshape(device_count, local_experts, CAP, -1)
    before = jnp.einsum(
        "sekd,edf->sekf",
        lax.all_to_all(outgoing, ("seq", "side"), split_axis=0, concat_axis=0, tiled=True),
        in_experts,
        preferred_element_type=jnp.float32,
    )
    hidden_sum = lax.psum(before, "req")
    hidden = jax.nn.silu(hidden_sum).astype(jnp.bfloat16)
    produced = jnp.einsum(
        "sekf,efd->sekd", hidden, out_experts, preferred_element_type=jnp.float32
    ).astype(jnp.bfloat16)
    came_back = lax.all_to_all(produced, ("seq", "side"), split_axis=0, concat_axis=0, tiled=True)
    slot_rows = came_back.reshape(slot_count, -1).astype(jnp.float32)
    expert_mix = jnp.dot(mixing.T, slot_rows, precision=lax.Precision.HIGHEST)
    return (attended, expert_mix.astype(jnp.bfloat16))


def solution(mesh):
    sizes = dict(mesh.shape)
    chips = sizes["seq"] // 2
    by_chips = (
        sizes["side"] == 1 and sizes["req"] == 2 and chips * (chips - 1) > 0 and chips & (chips - 1) == 0
    )

    def run(*operands):
        if by_chips and operands[0].shape[2] == chips:
            return device_by_chips(chips, *operands)
        return per_device(*operands)

    placed = (
        P(("groups", "req"), "seq", "side", None),
        P(("groups", "req"), "seq", "side"),
        P(("groups", "req"), "seq", "side"),
        P(("groups", "req"), "seq", "side"),
        P(("groups", "req"), "seq", "side"),
        P(("groups", "req"), None),
        P(("groups", "req")),
        P("side", "seq", "req"),
        P(("seq", "side"), "req", None),
        P(("seq", "side"), None, "req"),
        P(("groups", "seq", "side"), None),
        P(("groups", "seq", "side"), None),
    )
    return jax.shard_map(
        run,
        mesh=mesh,
        in_specs=placed,
        out_specs=(P(("groups", "seq", "side"), "req"), P(("groups", "seq", "side"), "req")),
        check_vma=False,
    )
```

```python
import math

import jax
import jax.numpy as jnp
from jax import lax
from jax.experimental import pallas as pl
from jax.experimental.pallas import tpu as pltpu
from jax.sharding import PartitionSpec as P


GROUP = 16
HD = 128
EXPERTS = 64
CAP = 6
NEG_FILL = -1e30
F32 = jnp.float32
BF16 = jnp.bfloat16


def call(body, outs, n_in, scratch=(), vmem=48 << 20, flops=1_000_000):
    return pl.pallas_call(
        body,
        out_shape=outs,
        in_specs=[pl.BlockSpec(memory_space=pltpu.SMEM)]
        + [pl.BlockSpec(memory_space=pltpu.VMEM)] * n_in,
        out_specs=jax.tree.map(lambda _: pl.BlockSpec(memory_space=pltpu.VMEM), outs),
        scratch_shapes=list(scratch),
        compiler_params=pltpu.CompilerParams(vmem_limit_bytes=vmem),
        cost_estimate=pl.CostEstimate(flops=flops, transcendentals=0, bytes_accessed=1_000_000),
    )


def shape(dims, kind=BF16):
    return jax.ShapeDtypeStruct(dims, kind)


def dot(a, b, dims=((1,), (0,))):
    return lax.dot_general(a, b, (dims, ((), ())), preferred_element_type=F32)


def pack_blocks(scalars, chips, queries, keys, tkeys, values, tvalues, experts, gates):
    nodes, width = queries.shape[1:]
    cached, tree = keys.shape[0], tkeys.shape[0]
    kv_rows = cached + tree
    cols = width // (2 * chips)
    top, per = experts.shape
    q_end = kv_rows + 2 * chips * nodes
    sources = (queries, keys, tkeys, values, tvalues)

    def body(s_ref, e_ref, g_ref, *refs):
        held = refs[len(sources) + chips : -1]
        sems = refs[-1]
        copies = [pltpu.make_async_copy(refs[n], held[n], sems.at[n]) for n in range(len(sources))]
        for copy in copies:
            copy.start()
        q_ref, k_ref, tk_ref, v_ref, tv_ref = held
        outs = refs[len(sources) : len(sources) + chips]
        z = s_ref[0]
        value = g_ref[...]
        high = value.astype(BF16)
        low = (value - high.astype(F32)).astype(BF16)
        row = lax.broadcasted_iota(jnp.int32, (top, cols), 0)
        col = lax.broadcasted_iota(jnp.int32, (top, cols), 1)
        route = jnp.zeros((per, cols), F32)
        for n, part in enumerate((e_ref[...].astype(F32).astype(BF16), high, low)):
            route += dot(part, (col == row + n * top).astype(F32).astype(BF16), ((0,), (0,)))
        for k in range(chips):
            outs[k][q_end:] = route.astype(BF16)
        for copy in copies:
            copy.wait()
        for k in range(chips):
            zk = z ^ k
            lanes = pl.ds(pl.multiple_of(zk * HD, HD), HD)
            out = outs[k]
            out[:cached, :HD] = k_ref[:, lanes]
            out[cached:kv_rows, :HD] = tk_ref[:, lanes]
            out[:cached, HD:] = v_ref[:, lanes]
            out[cached:kv_rows, HD:] = tv_ref[:, lanes]
            for n in range(2 * chips):
                at = kv_rows + n * nodes
                out[at : at + nodes] = q_ref[zk, :, n * cols : (n + 1) * cols]

    vmem, hbm = pl.BlockSpec(memory_space=pltpu.VMEM), pl.BlockSpec(memory_space=pltpu.HBM)
    return pl.pallas_call(
        body,
        out_shape=[shape((q_end + per, cols))] * chips,
        in_specs=[pl.BlockSpec(memory_space=pltpu.SMEM), vmem, vmem] + [hbm] * len(sources),
        out_specs=[vmem] * chips,
        scratch_shapes=[pltpu.VMEM(a.shape, a.dtype) for a in sources]
        + [pltpu.SemaphoreType.DMA((len(sources),))],
        compiler_params=pltpu.CompilerParams(vmem_limit_bytes=8 << 20),
        cost_estimate=pl.CostEstimate(flops=1_000_000, transcendentals=0, bytes_accessed=1_000_000),
    )(scalars, experts, gates, *sources)


def visibility(scalars, chips, cached, tree, parent_row):
    total = 2 * chips * tree
    ctx = 2 * chips * cached
    turns = max(1, (total - 1).bit_length())

    def body(s_ref, p_hbm, out, p_ref, sem):
        copy = pltpu.make_async_copy(p_hbm, p_ref, sem)
        copy.start()
        z, c, length = s_ref[0], s_ref[1], s_ref[2]
        copy.wait()
        rows = lax.broadcasted_iota(jnp.int32, (total, total), 0)
        cols = lax.broadcasted_iota(jnp.int32, (total, total), 1)
        hit = (jnp.broadcast_to(p_ref[...], (total, total)) == rows) | (rows == cols)
        reach = hit.astype(F32).astype(BF16)
        for _ in range(turns):
            reach = jnp.minimum(dot(reach, reach), 1.0).astype(BF16)
        block = rows // tree
        node = (((z ^ (block >> 1)) << 1) | (c ^ (block & 1))) * tree + rows % tree
        order = (node == cols).astype(F32).astype(BF16)
        left = dot(order, reach, ((1,), (1,))).astype(BF16)
        seen = dot(left, order, ((1,), (1,)))
        out[:, ctx:] = jnp.where(seen > 0.5, 0.0, NEG_FILL)
        lane = lax.broadcasted_iota(jnp.int32, (total, ctx), 1)
        block = lane // cached
        place = (((z ^ (block >> 1)) << 1) | (c ^ (block & 1))) * cached + lane % cached
        out[:, :ctx] = jnp.where(place < length, 0.0, NEG_FILL)

    return pl.pallas_call(
        body,
        out_shape=shape((total, ctx + total), F32),
        in_specs=[pl.BlockSpec(memory_space=pltpu.SMEM), pl.BlockSpec(memory_space=pltpu.HBM)],
        out_specs=pl.BlockSpec(memory_space=pltpu.VMEM),
        scratch_shapes=[pltpu.VMEM(parent_row.shape, parent_row.dtype), pltpu.SemaphoreType.DMA],
        compiler_params=pltpu.CompilerParams(vmem_limit_bytes=8 << 20),
        cost_estimate=pl.CostEstimate(flops=40_000_000, transcendentals=0, bytes_accessed=1_000_000),
    )(scalars, parent_row)


def attend(scalars, chips, cached, tree, own, partner, bias):
    total, width = bias.shape
    ctx = 2 * chips * cached
    kv_rows = cached + tree
    q_rows = total // chips
    per = own[0].shape[1] // HD
    factor = 1.0 / math.sqrt(HD)

    def body(s_ref, *refs):
        blocks = (refs[:chips], refs[chips : 2 * chips])
        b_ref = refs[2 * chips]
        outs = refs[2 * chips + 1 : 3 * chips + 1]
        keys, values, rows = refs[3 * chips + 1 :]
        z, c = s_ref[0], s_ref[1]
        for k in range(chips):
            for t in range(2):
                b, src = 2 * k + t, blocks[t][k]
                for dst, cols in ((keys, slice(0, HD)), (values, slice(HD, 2 * HD))):
                    dst[b * cached : (b + 1) * cached] = src[:cached, cols]
                    dst[ctx + b * tree : ctx + (b + 1) * tree] = src[cached:kv_rows, cols]
        for kk in range(chips):
            at = pl.ds(pl.multiple_of(kv_rows + (2 * (z ^ kk) + c) * tree, 16), tree)
            for j in range(per):
                for k in range(chips):
                    for t in range(2):
                        first = j * total + k * q_rows + t * tree
                        rows[first : first + tree] = blocks[t][k][at, j * HD : (j + 1) * HD]
            scores = dot(rows[...], keys[...], ((1,), (1,))) * factor
            scores = (scores.reshape(per, total, width) + b_ref[...][None]).reshape(per * total, width)
            top = jnp.max(scores, axis=-1, keepdims=True)
            weights = jnp.exp(scores - top)
            mass = jnp.sum(weights, axis=-1, keepdims=True)
            result = (dot(weights.astype(BF16), values[...]) / mass).astype(BF16)
            for j in range(per):
                for k in range(chips):
                    for t in range(2):
                        first = j * total + k * q_rows + t * tree
                        node = pl.multiple_of((((z ^ k) << 1) | (c ^ t)) * tree, 16)
                        outs[kk][pl.ds(node, tree), j * HD : (j + 1) * HD] = result[first : first + tree]

    return call(
        body,
        [shape((total, per * HD))] * chips,
        2 * chips + 1,
        [pltpu.VMEM((width, HD), BF16), pltpu.VMEM((width, HD), BF16), pltpu.VMEM((per * total, HD), BF16)],
        flops=4 * per * chips * total * width * HD,
    )(scalars, *own, *partner, bias)


def project(scalars, chips, turn, blocks, weight, done=(), tile=512):
    rows, depth = blocks[0].shape
    cols = weight.shape[2]
    block = rows // chips
    half = chips // 2
    tiles = cols // tile

    def body(s_ref, *refs):
        w_ref = refs[chips]
        earlier = refs[chips + 1 : chips + 1 + len(done)]
        mine, theirs = refs[chips + 1 + len(done) : chips + 3 + len(done)]
        z, c, x = s_ref[0], s_ref[1], s_ref[3]
        copies = []
        if not done:
            held, sems = refs[-2], refs[-1]
            copies = [
                pltpu.make_async_copy(
                    w_ref.at[:, :, pl.ds(n * tile, tile)], held.at[:, :, pl.ds(n * tile, tile)], sems.at[n]
                )
                for n in range(tiles)
            ]
            w_ref = held
        for copy in copies:
            copy.start()
        for m in range(half if done else 0):
            before = z ^ ((x ^ turn ^ 1) * half + m)
            mine[before] = earlier[0][m]
            theirs[before] = earlier[1][m]
        for n in range(tiles):
            lanes = slice(n * tile, (n + 1) * tile)
            if copies:
                copies[n].wait()
            total = None
            for k in range(chips):
                part = dot(refs[k][...], w_ref[z ^ k, :, lanes])
                total = part if total is None else total + part
            for m in range(half):
                at = z ^ ((x ^ turn) * half + m) if done else m
                low = total[2 * m * block : (2 * m + 1) * block]
                high = total[(2 * m + 1) * block : (2 * m + 2) * block]
                mine[at, :, lanes] = jnp.where(c == 0, low, high)
                theirs[at, :, lanes] = jnp.where(c == 0, high, low).astype(BF16)

    count = chips if done else half
    vmem = pl.BlockSpec(memory_space=pltpu.VMEM)
    outs = (shape((count, block, cols), F32), shape((count, block, cols)))
    if not done:
        outs += (shape(weight.shape),)
    return pl.pallas_call(
        body,
        out_shape=outs,
        in_specs=[pl.BlockSpec(memory_space=pltpu.SMEM)]
        + [vmem] * chips
        + [vmem if done else pl.BlockSpec(memory_space=pltpu.HBM)]
        + [vmem] * len(done),
        out_specs=(vmem,) * len(outs),
        scratch_shapes=[] if done else [pltpu.SemaphoreType.DMA((tiles,))],
        compiler_params=pltpu.CompilerParams(vmem_limit_bytes=16 << 20),
        cost_estimate=pl.CostEstimate(
            flops=2 * rows * chips * depth * cols, transcendentals=0, bytes_accessed=2 * weight.size
        ),
    )(scalars, *blocks, weight, *done)


def routing(scalars, chips, own, partner, local, slots, top, first_row):
    per = own[0].shape[0] - first_row
    tokens = 2 * chips * per
    count = local * slots

    def body(s_ref, *refs):
        pick, gate, table = refs[2 * chips], refs[2 * chips + 1], refs[2 * chips + 2]
        base = s_ref[4].astype(F32)
        for k in range(chips):
            for t in range(2):
                b = 2 * k + t
                table[b * per : (b + 1) * per] = refs[t * chips + k][first_row:, :HD].astype(F32)
        lane = lax.broadcasted_iota(jnp.int32, (tokens, HD), 1)
        expert = jnp.where(lane < local, base + lane.astype(F32), -1.0)
        zero = jnp.zeros((tokens, HD), F32)
        hit, high, low = zero, zero, zero
        for n in range(top):
            same = table[:, n : n + 1] == expert
            hit = jnp.where(same, 1.0, hit)
            high = jnp.where(same, table[:, top + n : top + n + 1], high)
            low = jnp.where(same, table[:, 2 * top + n : 2 * top + n + 1], low)
        earlier = lax.broadcasted_iota(jnp.int32, (tokens, tokens), 1) < lax.broadcasted_iota(
            jnp.int32, (tokens, tokens), 0
        )
        rank = dot(earlier.astype(F32).astype(BF16), hit.astype(BF16))
        row = lax.broadcasted_iota(jnp.int32, (HD, count), 0)
        col = lax.broadcasted_iota(jnp.int32, (HD, count), 1)
        spread = ((col >= row * slots) & (col < (row + 1) * slots)).astype(F32).astype(BF16)
        hit_at = dot(hit.astype(BF16), spread)
        rank_at = dot(rank.astype(BF16), spread)
        slot = (lax.broadcasted_iota(jnp.int32, (tokens, count), 1) % slots).astype(F32)
        placed = ((hit_at > 0.5) & (rank_at == slot)).astype(F32)
        placing = placed.T.astype(BF16)
        pick[...] = placing
        weights = dot(placing, high.astype(BF16)) + dot(placing, low.astype(BF16))
        mine = lax.broadcasted_iota(jnp.int32, (count, HD), 0) // slots == lax.broadcasted_iota(
            jnp.int32, (count, HD), 1
        )
        total = jnp.sum(jnp.where(mine, weights, 0.0), axis=1, keepdims=True)
        gate[...] = jnp.broadcast_to(total, (count, HD))

    return call(
        body,
        (shape((count, tokens)), shape((count, HD), F32)),
        2 * chips,
        [pltpu.VMEM((tokens, HD), F32)],
        flops=100_000_000,
    )(scalars, *own, *partner)


def stream(body, operands, weight, first, experts, out, piece, scratch):
    depth, width = weight.shape[1:]
    pieces = depth // piece
    total = len(operands)

    def kernel(*refs):
        w_ref, out_ref, held, sems = refs[total], refs[total + 1], refs[-2], refs[-1]

        def part(e, n):
            rows = pl.ds(n * piece, piece)
            return pltpu.make_async_copy(w_ref.at[first + e, rows], held.at[e, rows], sems.at[e, n])

        for e in range(experts):
            for n in range(pieces):
                part(e, n).start()

        def product(rows, e):
            total = None
            for n in range(pieces):
                part(e, n).wait()
                at = slice(n * piece, (n + 1) * piece)
                more = dot(rows[:, at], held[e, at])
                total = more if total is None else total + more
            return total

        body(refs[:total], out_ref, refs[total + 2 : -2], product)

    vmem = pl.BlockSpec(memory_space=pltpu.VMEM)
    return pl.pallas_call(
        kernel,
        out_shape=out,
        in_specs=[vmem] * total + [pl.BlockSpec(memory_space=pltpu.HBM)],
        out_specs=vmem,
        scratch_shapes=list(scratch)
        + [
            pltpu.VMEM((experts, depth, width), BF16),
            pltpu.SemaphoreType.DMA((experts, pieces)),
        ],
        compiler_params=pltpu.CompilerParams(vmem_limit_bytes=24 << 20),
        cost_estimate=pl.CostEstimate(
            flops=2 * out.shape[0] * depth * width,
            transcendentals=0,
            bytes_accessed=2 * experts * depth * width,
        ),
    )(*operands, weight)


def expert_in(chips, own, partner, pick, weight, first, experts, slots):
    rows, depth = own[0].shape
    tokens = 2 * chips * rows

    def body(refs, out, scratch, product):
        table, picked = scratch
        for k in range(chips):
            for t in range(2):
                b = 2 * k + t
                table[b * rows : (b + 1) * rows] = refs[t * chips + k][...]
        at = slice(first * slots, (first + experts) * slots)
        picked[...] = dot(refs[-1][at], table[...]).astype(BF16)
        for e in range(experts):
            at = slice(e * slots, (e + 1) * slots)
            out[at] = product(picked[at], e).astype(BF16)

    return stream(
        body, (*own, *partner, pick), weight, first, experts, shape((experts * slots, weight.shape[2])),
        depth // 4, [pltpu.VMEM((tokens, depth), BF16), pltpu.VMEM((experts * slots, depth), BF16)],
    )


def expert_out(before, before_other, gate, weight, first, experts, slots):
    def body(refs, out, scratch, product):
        a_ref, b_ref, g_ref = refs
        for e in range(experts):
            at = slice(e * slots, (e + 1) * slots)
            total = a_ref[at].astype(F32) + b_ref[at].astype(F32)
            gates = g_ref[(first + e) * slots : (first + e + 1) * slots, :1]
            hidden = total / (1.0 + jnp.exp(-total)) * gates
            out[at] = product(hidden.astype(BF16), e).astype(BF16)

    return stream(
        body, (before, before_other, gate), weight, first, experts,
        shape((experts * slots, weight.shape[2])), weight.shape[1] // 4, [],
    )


def combine(chips, pick, produced, tile=512):
    count, tokens = pick.shape
    chunks = len(produced)
    step, cols = produced[0].shape
    rows = tokens // (2 * chips)

    def body(p_ref, *refs):
        mine, theirs = refs[chunks:]
        total = None
        for n in range(chunks):
            part = dot(p_ref[n * step : (n + 1) * step], refs[n][...], ((0,), (0,)))
            total = part if total is None else total + part
        for k in range(chips):
            at = 2 * k * rows
            mine[k] = total[at : at + rows]
            theirs[k] = total[at + rows : at + 2 * rows].astype(BF16)

    return pl.pallas_call(
        body,
        grid=(cols // tile,),
        out_shape=(shape((chips, rows, cols), F32), shape((chips, rows, cols))),
        in_specs=[pl.BlockSpec((count, tokens), lambda n: (0, 0))]
        + [pl.BlockSpec((step, tile), lambda n: (0, n))] * chunks,
        out_specs=(pl.BlockSpec((chips, rows, tile), lambda n: (0, 0, n)),) * 2,
        compiler_params=pltpu.CompilerParams(vmem_limit_bytes=32 << 20),
        cost_estimate=pl.CostEstimate(
            flops=2 * count * tokens * cols, transcendentals=0, bytes_accessed=4 * count * cols
        ),
    )(pick, *produced)


def device_by_chips(
    chips,
    queries,
    cache_keys,
    cache_values,
    tree_keys,
    tree_values,
    parents,
    lengths,
    out_weight,
    in_experts,
    out_experts,
    gate_experts,
    gate_weights,
):
    count = 2 * chips
    index = lax.axis_index("seq")
    chip, core = index // 2, index % 2
    local = in_experts.shape[0]
    top = gate_experts.shape[1]
    slots = count * CAP
    cached, tree = cache_keys.shape[1], tree_keys.shape[1]
    scalars = jnp.stack(
        [chip, core, lengths[0], lax.axis_index("req"), index * local]
    ).astype(jnp.int32)

    def to_partner(a):
        return lax.ppermute(a, "seq", [(i, i ^ 1) for i in range(count)])

    def to_chip(a, k):
        return lax.ppermute(a, "seq", [(i, i ^ (2 * k)) for i in range(count)])

    def over_req(a):
        return lax.ppermute(a, "req", [(0, 1), (1, 0)])

    def scatter_sum(mine, theirs):
        paired = mine + to_partner(theirs).astype(F32)
        sent = [to_chip(paired[k].astype(BF16), k) for k in range(1, chips)]
        total = paired[0]
        for piece in sent:
            total = total + piece.astype(F32)
        return total.astype(BF16)

    packed = pack_blocks(
        scalars, chips, queries[0].transpose(1, 0, 2), cache_keys[0], tree_keys[0], cache_values[0], tree_values[0],
        gate_experts.T, gate_weights.T,
    )
    own = [packed[0]] + [to_chip(packed[k], k) for k in range(1, chips)]
    partner = [to_partner(block) for block in own]
    bias = visibility(scalars, chips, cached, tree, parents)
    first_row = packed[0].shape[0] - gate_experts.shape[0]
    pick, gate = routing(scalars, chips, own, partner, local, slots, top, first_row)
    results = attend(scalars, chips, cached, tree, own, partner, bias)
    results = [results[0]] + [to_chip(results[k], k) for k in range(1, chips)]
    swapped = [over_req(block) for block in results]
    *here, held = project(scalars, chips, 0, results, out_weight)
    attended = scatter_sum(*project(scalars, chips, 1, swapped, held, here))
    rows = [attended] + [to_chip(attended, k) for k in range(1, chips)]
    rows_partner = [to_partner(block) for block in rows]
    step = max(1, local // 4)
    before = [
        expert_in(chips, rows, rows_partner, pick, in_experts, first, step, slots)
        for first in range(0, local, step)
    ]
    before_other = [over_req(part) for part in before]
    produced = [
        expert_out(before[n], before_other[n], gate, out_experts, n * step, step, slots)
        for n in range(len(before))
    ]
    return (attended, scatter_sum(*combine(chips, pick, produced)))


def ancestors(parent_row, node_count):
    node_ids = jnp.arange(node_count, dtype=jnp.int32)
    parent_hit = (node_ids[None, :] == parent_row[:, None]).astype(jnp.float32)
    reached = jnp.maximum(parent_hit, jnp.eye(node_count, dtype=jnp.float32))
    for _ in range(max(1, (node_count - 1).bit_length())):
        reached = jnp.minimum(jnp.dot(reached, reached, precision=lax.Precision.HIGHEST), 1.0)
    return reached


def per_device(
    queries,
    cache_keys,
    cache_values,
    tree_keys,
    tree_values,
    parents,
    lengths,
    out_weight,
    in_experts,
    out_experts,
    gate_experts,
    gate_weights,
):
    seq_index = lax.axis_index("seq")
    ctx_local = cache_keys.shape[1]
    nodes_local = queries.shape[1]
    kv_local = queries.shape[2]
    gathered = lax.all_gather(queries, "seq", axis=1, tiled=True)
    node_count = gathered.shape[1]
    reached = ancestors(parents[0], node_count)
    tree_seen = lax.dynamic_slice_in_dim(reached, seq_index * nodes_local, nodes_local, 1) > 0.5
    positions = seq_index * ctx_local + jnp.arange(ctx_local, dtype=jnp.int32)
    context_seen = jnp.broadcast_to((positions < lengths[0])[None, :], (node_count, ctx_local))
    visible = jnp.concatenate([context_seen, tree_seen], axis=1)[None]
    factor = 1.0 / math.sqrt(HD)
    outputs, maxima, totals = ([], [], [])
    for head_pair in range(kv_local):
        first_col = head_pair * HD
        key_rows = jnp.concatenate(
            [
                cache_keys[0, :, first_col : first_col + HD],
                tree_keys[0, :, first_col : first_col + HD],
            ],
            axis=0,
        )
        value_rows = jnp.concatenate(
            [
                cache_values[0, :, first_col : first_col + HD],
                tree_values[0, :, first_col : first_col + HD],
            ],
            axis=0,
        )
        query_block = gathered[0, :, head_pair].reshape(node_count, GROUP, HD)
        scores = (
            jnp.einsum("ngd,kd->gnk", query_block, key_rows, preferred_element_type=jnp.float32)
            * factor
        )
        masked = jnp.where(visible, scores, NEG_FILL)
        row_max = jnp.max(masked, axis=-1)
        weights = jnp.where(visible, jnp.exp(masked - row_max[..., None]), 0.0)
        weights_low = weights.astype(jnp.bfloat16)
        outputs.append(
            jnp.einsum("gnk,kd->gnd", weights_low, value_rows, preferred_element_type=jnp.float32)
        )
        maxima.append(row_max)
        totals.append(jnp.sum(weights, axis=-1))
    partial_out = jnp.stack(outputs)
    partial_max = jnp.stack(maxima)
    partial_sum = jnp.stack(totals)
    pieces = (
        lax.all_to_all(partial_out[None], "seq", split_axis=2, concat_axis=0, tiled=True),
        lax.all_to_all(partial_max[None], "seq", split_axis=2, concat_axis=0, tiled=True),
        lax.all_to_all(partial_sum[None], "seq", split_axis=2, concat_axis=0, tiled=True),
    )
    larger = jnp.max(pieces[1], axis=0)
    scales = jnp.exp(pieces[1] - larger[None])
    merged = jnp.sum(pieces[0] * scales[..., None], axis=0)
    summed = jnp.sum(pieces[2] * scales, axis=0)
    attention = merged / summed[..., None]
    attention = jnp.transpose(attention, (2, 0, 1, 3)).reshape(node_count, -1).astype(jnp.bfloat16)
    head_rows = lax.all_gather(attention, "req", axis=0, tiled=True)
    projector = out_weight.reshape(-1, out_weight.shape[2])
    attended = lax.psum_scatter(
        jnp.dot(head_rows, projector, preferred_element_type=jnp.float32),
        ("seq", "side"),
        scatter_dimension=0,
        tiled=True,
    ).astype(jnp.bfloat16)
    local_experts = in_experts.shape[0]
    flat_ids = gate_experts.reshape(-1)
    expert_hit = (flat_ids[:, None] == jnp.arange(EXPERTS, dtype=jnp.int32)[None, :]).astype(
        jnp.int32
    )
    earlier = jnp.cumsum(expert_hit, axis=0) - expert_hit
    slot_rank = jnp.sum(earlier * expert_hit, axis=1)
    slot_ids = (flat_ids * CAP + slot_rank).reshape(gate_experts.shape)
    slot_count = EXPERTS * CAP
    matches = jnp.arange(slot_count, dtype=jnp.int32)[:, None, None] == slot_ids[None]
    placing = jnp.any(matches, axis=2).astype(jnp.bfloat16)
    mixing = jnp.sum(jnp.where(matches, gate_weights[None], 0.0), axis=2)
    outgoing = jnp.dot(placing, attended, preferred_element_type=jnp.float32).astype(jnp.bfloat16)
    device_count = EXPERTS // local_experts
    outgoing = outgoing.reshape(device_count, local_experts, CAP, -1)
    before = jnp.einsum(
        "sekd,edf->sekf",
        lax.all_to_all(outgoing, ("seq", "side"), split_axis=0, concat_axis=0, tiled=True),
        in_experts,
        preferred_element_type=jnp.float32,
    )
    hidden_sum = lax.psum(before, "req")
    hidden = jax.nn.silu(hidden_sum).astype(jnp.bfloat16)
    produced = jnp.einsum(
        "sekf,efd->sekd", hidden, out_experts, preferred_element_type=jnp.float32
    ).astype(jnp.bfloat16)
    came_back = lax.all_to_all(produced, ("seq", "side"), split_axis=0, concat_axis=0, tiled=True)
    slot_rows = came_back.reshape(slot_count, -1).astype(jnp.float32)
    expert_mix = jnp.dot(mixing.T, slot_rows, precision=lax.Precision.HIGHEST)
    return (attended, expert_mix.astype(jnp.bfloat16))


def solution(mesh):
    sizes = dict(mesh.shape)
    chips = sizes["seq"] // 2
    by_chips = (
        sizes["side"] == 1 and sizes["req"] == 2 and chips * (chips - 1) > 0 and chips & (chips - 1) == 0
    )

    def run(*operands):
        if by_chips and operands[0].shape[2] == chips:
            return device_by_chips(chips, *operands)
        return per_device(*operands)

    placed = (
        P(("groups", "req"), "seq", "side", None),
        P(("groups", "req"), "seq", "side"),
        P(("groups", "req"), "seq", "side"),
        P(("groups", "req"), "seq", "side"),
        P(("groups", "req"), "seq", "side"),
        P(("groups", "req"), None),
        P(("groups", "req")),
        P("side", "seq", "req"),
        P(("seq", "side"), "req", None),
        P(("seq", "side"), None, "req"),
        P(("groups", "seq", "side"), None),
        P(("groups", "seq", "side"), None),
    )
    return jax.shard_map(
        run,
        mesh=mesh,
        in_specs=placed,
        out_specs=(P(("groups", "seq", "side"), "req"), P(("groups", "seq", "side"), "req")),
        check_vma=False,
    )
```

```python
import math

import jax
import jax.numpy as jnp
from jax import lax
from jax.experimental import pallas as pl
from jax.experimental.pallas import tpu as pltpu
from jax.sharding import PartitionSpec as P


GROUP = 16
HD = 128
EXPERTS = 64
CAP = 6
NEG_FILL = -1e30
CHUNKS = 4
F32 = jnp.float32
BF16 = jnp.bfloat16


def call(body, outs, n_in, scratch=(), vmem=12 << 20, flops=1_000_000):
    return pl.pallas_call(
        body,
        out_shape=outs,
        in_specs=[pl.BlockSpec(memory_space=pltpu.SMEM)]
        + [pl.BlockSpec(memory_space=pltpu.VMEM)] * n_in,
        out_specs=jax.tree.map(lambda _: pl.BlockSpec(memory_space=pltpu.VMEM), outs),
        scratch_shapes=list(scratch),
        compiler_params=pltpu.CompilerParams(vmem_limit_bytes=vmem),
        cost_estimate=pl.CostEstimate(flops=flops, transcendentals=0, bytes_accessed=1_000_000),
    )


def shape(dims, kind=BF16):
    return jax.ShapeDtypeStruct(dims, kind)


def in_hbm(a):
    return pltpu.with_memory_space_constraint(a, pltpu.HBM)


PIECES = 4


def pieces_of(source, first, held, sems):
    count, depth = held.shape[:2]
    piece = depth // PIECES
    return [
        pltpu.make_async_copy(
            source.at[first + n, pl.ds(m * piece, piece)], held.at[n, pl.ds(m * piece, piece)], sems.at[n, m]
        )
        for n in range(count)
        for m in range(PIECES)
    ]


def fetch(weight, first, count):
    def body(w_ref, out, sems):
        copies = pieces_of(w_ref, first, out, sems)
        for copy in copies:
            copy.start()
        for copy in copies:
            copy.wait()

    dims = (count,) + weight.shape[1:]
    return pl.pallas_call(
        body,
        out_shape=pltpu.VMEM(dims, BF16),
        in_specs=[pl.BlockSpec(memory_space=pltpu.HBM)],
        out_specs=pl.BlockSpec(memory_space=pltpu.VMEM),
        scratch_shapes=[pltpu.SemaphoreType.DMA((count, PIECES))],
        compiler_params=pltpu.CompilerParams(vmem_limit_bytes=1 << 20),
        cost_estimate=pl.CostEstimate(flops=1_000_000, transcendentals=0, bytes_accessed=2 * math.prod(dims)),
    )(in_hbm(weight))


def dot(a, b, dims=((1,), (0,))):
    return lax.dot_general(a, b, (dims, ((), ())), preferred_element_type=F32)


def pack_blocks(scalars, chips, queries, keys, tkeys, values, tvalues, experts, gates):
    nodes, width = queries.shape[1:]
    cached, tree = keys.shape[0], tkeys.shape[0]
    kv_rows = cached + tree
    cols = width // (2 * chips)
    top, per = experts.shape
    q_end = kv_rows + 2 * chips * nodes
    sources = (experts, gates, queries, keys, tkeys, values, tvalues)

    def body(s_ref, *refs):
        held = refs[len(sources) + chips : -1]
        sems = refs[-1]
        copies = [pltpu.make_async_copy(refs[n], held[n], sems.at[n]) for n in range(len(sources))]
        for copy in copies:
            copy.start()
        e_ref, g_ref, q_ref, k_ref, tk_ref, v_ref, tv_ref = held
        outs = refs[len(sources) : len(sources) + chips]
        z = s_ref[0]
        for copy in copies[:2]:
            copy.wait()
        value = g_ref[...]
        high = value.astype(BF16)
        low = (value - high.astype(F32)).astype(BF16)
        row = lax.broadcasted_iota(jnp.int32, (top, cols), 0)
        col = lax.broadcasted_iota(jnp.int32, (top, cols), 1)
        route = jnp.zeros((per, cols), F32)
        for n, part in enumerate((e_ref[...].astype(F32).astype(BF16), high, low)):
            route += dot(part, (col == row + n * top).astype(F32).astype(BF16), ((0,), (0,)))
        for k in range(chips):
            outs[k][q_end:] = route.astype(BF16)
        for copy in copies[2:]:
            copy.wait()
        for k in range(chips):
            zk = z ^ k
            lanes = pl.ds(pl.multiple_of(zk * HD, HD), HD)
            out = outs[k]
            out[:cached, :HD] = k_ref[:, lanes]
            out[cached:kv_rows, :HD] = tk_ref[:, lanes]
            out[:cached, HD:] = v_ref[:, lanes]
            out[cached:kv_rows, HD:] = tv_ref[:, lanes]
            for n in range(2 * chips):
                at = kv_rows + n * nodes
                out[at : at + nodes] = q_ref[zk, :, n * cols : (n + 1) * cols]

    vmem, hbm = pl.BlockSpec(memory_space=pltpu.VMEM), pl.BlockSpec(memory_space=pltpu.HBM)
    return pl.pallas_call(
        body,
        out_shape=[shape((q_end + per, cols))] * chips,
        in_specs=[pl.BlockSpec(memory_space=pltpu.SMEM)] + [hbm] * len(sources),
        out_specs=[vmem] * chips,
        scratch_shapes=[pltpu.VMEM(a.shape, a.dtype) for a in sources]
        + [pltpu.SemaphoreType.DMA((len(sources),))],
        compiler_params=pltpu.CompilerParams(vmem_limit_bytes=8 << 20),
        cost_estimate=pl.CostEstimate(flops=1_000_000, transcendentals=0, bytes_accessed=1_000_000),
    )(scalars, *map(in_hbm, sources))


def visibility(scalars, chips, cached, tree, parent_row):
    total = 2 * chips * tree
    ctx = 2 * chips * cached
    turns = max(1, (total - 1).bit_length())

    def body(s_ref, p_hbm, out, p_ref, sem):
        copy = pltpu.make_async_copy(p_hbm, p_ref, sem)
        copy.start()
        z, c, length = s_ref[0], s_ref[1], s_ref[2]
        copy.wait()
        rows = lax.broadcasted_iota(jnp.int32, (total, total), 0)
        cols = lax.broadcasted_iota(jnp.int32, (total, total), 1)
        hit = (jnp.broadcast_to(p_ref[...], (total, total)) == rows) | (rows == cols)
        reach = hit.astype(F32).astype(BF16)
        for _ in range(turns):
            reach = jnp.minimum(dot(reach, reach), 1.0).astype(BF16)
        block = rows // tree
        node = (((z ^ (block >> 1)) << 1) | (c ^ (block & 1))) * tree + rows % tree
        order = (node == cols).astype(F32).astype(BF16)
        left = dot(order, reach, ((1,), (1,))).astype(BF16)
        seen = dot(left, order, ((1,), (1,)))
        out[:, ctx:] = jnp.where(seen > 0.5, 0.0, NEG_FILL)
        lane = lax.broadcasted_iota(jnp.int32, (total, ctx), 1)
        block = lane // cached
        place = (((z ^ (block >> 1)) << 1) | (c ^ (block & 1))) * cached + lane % cached
        out[:, :ctx] = jnp.where(place < length, 0.0, NEG_FILL)

    return pl.pallas_call(
        body,
        out_shape=shape((total, ctx + total), F32),
        in_specs=[pl.BlockSpec(memory_space=pltpu.SMEM), pl.BlockSpec(memory_space=pltpu.HBM)],
        out_specs=pl.BlockSpec(memory_space=pltpu.VMEM),
        scratch_shapes=[pltpu.VMEM(parent_row.shape, parent_row.dtype), pltpu.SemaphoreType.DMA],
        compiler_params=pltpu.CompilerParams(vmem_limit_bytes=8 << 20),
        cost_estimate=pl.CostEstimate(flops=40_000_000, transcendentals=0, bytes_accessed=1_000_000),
    )(scalars, in_hbm(parent_row))


def attend(scalars, chips, cached, tree, own, partner, bias, wanted):
    total, width = bias.shape
    ctx = 2 * chips * cached
    kv_rows = cached + tree
    q_rows = total // chips
    per = own[0].shape[1] // HD
    factor = 1.0 / math.sqrt(HD)

    def body(s_ref, *refs):
        blocks = (refs[:chips], refs[chips : 2 * chips])
        b_ref = refs[2 * chips]
        outs = refs[2 * chips + 1 : 2 * chips + 1 + len(wanted)]
        keys, values, rows = refs[2 * chips + 1 + len(wanted) :]
        z, c = s_ref[0], s_ref[1]
        for k in range(chips):
            for t in range(2):
                b, src = 2 * k + t, blocks[t][k]
                for dst, cols in ((keys, slice(0, HD)), (values, slice(HD, 2 * HD))):
                    dst[b * cached : (b + 1) * cached] = src[:cached, cols]
                    dst[ctx + b * tree : ctx + (b + 1) * tree] = src[cached:kv_rows, cols]
        for out, kk in zip(outs, wanted, strict=True):
            at = pl.ds(pl.multiple_of(kv_rows + (2 * (z ^ kk) + c) * tree, 16), tree)
            for j in range(per):
                for k in range(chips):
                    for t in range(2):
                        first = j * total + k * q_rows + t * tree
                        rows[first : first + tree] = blocks[t][k][at, j * HD : (j + 1) * HD]
            scores = dot(rows[...], keys[...], ((1,), (1,))) * factor
            scores = (scores.reshape(per, total, width) + b_ref[...][None]).reshape(per * total, width)
            top = jnp.max(scores, axis=-1, keepdims=True)
            weights = jnp.exp(scores - top)
            mass = jnp.sum(weights, axis=-1, keepdims=True)
            result = (dot(weights.astype(BF16), values[...]) / mass).astype(BF16)
            for j in range(per):
                for k in range(chips):
                    for t in range(2):
                        first = j * total + k * q_rows + t * tree
                        node = pl.multiple_of((((z ^ k) << 1) | (c ^ t)) * tree, 16)
                        out[pl.ds(node, tree), j * HD : (j + 1) * HD] = result[first : first + tree]

    return call(
        body,
        [shape((total, per * HD))] * len(wanted),
        2 * chips + 1,
        [pltpu.VMEM((width, HD), BF16), pltpu.VMEM((width, HD), BF16), pltpu.VMEM((per * total, HD), BF16)],
        flops=4 * per * len(wanted) * total * width * HD,
    )(scalars, *own, *partner, bias)


def project(scalars, chips, turn, blocks, weight, done=(), tile=512):
    rows, depth = blocks[0].shape
    cols = weight.shape[2]
    block = rows // chips
    half = chips // 2
    tiles = cols // tile

    def body(s_ref, *refs):
        w_ref = refs[chips]
        earlier = refs[chips + 1 : chips + 1 + len(done)]
        mine, theirs = refs[chips + 1 + len(done) : chips + 3 + len(done)]
        z, c, x = s_ref[0], s_ref[1], s_ref[3]
        for m in range(half if done else 0):
            before = z ^ ((x ^ turn ^ 1) * half + m)
            mine[before] = earlier[0][m]
            theirs[before] = earlier[1][m]
        for n in range(tiles):
            lanes = slice(n * tile, (n + 1) * tile)
            total = None
            for k in range(chips):
                part = dot(refs[k][...], w_ref[z ^ k, :, lanes])
                total = part if total is None else total + part
            for m in range(half):
                at = z ^ ((x ^ turn) * half + m) if done else m
                low = total[2 * m * block : (2 * m + 1) * block]
                high = total[(2 * m + 1) * block : (2 * m + 2) * block]
                mine[at, :, lanes] = jnp.where(c == 0, low, high)
                theirs[at, :, lanes] = jnp.where(c == 0, high, low).astype(BF16)

    count = chips if done else half
    vmem = pl.BlockSpec(memory_space=pltpu.VMEM)
    outs = (shape((count, block, cols), F32), shape((count, block, cols)))
    return pl.pallas_call(
        body,
        out_shape=outs,
        in_specs=[pl.BlockSpec(memory_space=pltpu.SMEM)]
        + [vmem] * chips
        + [vmem]
        + [vmem] * len(done),
        out_specs=(vmem,) * len(outs),
        compiler_params=pltpu.CompilerParams(vmem_limit_bytes=10 << 20),
        cost_estimate=pl.CostEstimate(
            flops=2 * rows * chips * depth * cols, transcendentals=0, bytes_accessed=2 * weight.size
        ),
    )(scalars, *blocks, weight, *done)


def routing(scalars, chips, own, partner, local, slots, top, first_row):
    per = own[0].shape[0] - first_row
    tokens = 2 * chips * per
    count = local * slots

    def body(s_ref, *refs):
        pick, gate, table = refs[2 * chips], refs[2 * chips + 1], refs[2 * chips + 2]
        base = s_ref[4].astype(F32)
        for k in range(chips):
            for t in range(2):
                b = 2 * k + t
                table[b * per : (b + 1) * per] = refs[t * chips + k][first_row:, :HD].astype(F32)
        lane = lax.broadcasted_iota(jnp.int32, (tokens, HD), 1)
        expert = jnp.where(lane < local, base + lane.astype(F32), -1.0)
        zero = jnp.zeros((tokens, HD), F32)
        hit, high, low = zero, zero, zero
        for n in range(top):
            same = table[:, n : n + 1] == expert
            hit = jnp.where(same, 1.0, hit)
            high = jnp.where(same, table[:, top + n : top + n + 1], high)
            low = jnp.where(same, table[:, 2 * top + n : 2 * top + n + 1], low)
        earlier = lax.broadcasted_iota(jnp.int32, (tokens, tokens), 1) < lax.broadcasted_iota(
            jnp.int32, (tokens, tokens), 0
        )
        rank = dot(earlier.astype(F32).astype(BF16), hit.astype(BF16))
        row = lax.broadcasted_iota(jnp.int32, (HD, count), 0)
        col = lax.broadcasted_iota(jnp.int32, (HD, count), 1)
        spread = ((col >= row * slots) & (col < (row + 1) * slots)).astype(F32).astype(BF16)
        hit_at = dot(hit.astype(BF16), spread)
        rank_at = dot(rank.astype(BF16), spread)
        slot = (lax.broadcasted_iota(jnp.int32, (tokens, count), 1) % slots).astype(F32)
        placed = ((hit_at > 0.5) & (rank_at == slot)).astype(F32)
        placing = placed.T.astype(BF16)
        pick[...] = placing
        weights = dot(placing, high.astype(BF16)) + dot(placing, low.astype(BF16))
        mine = lax.broadcasted_iota(jnp.int32, (count, HD), 0) // slots == lax.broadcasted_iota(
            jnp.int32, (count, HD), 1
        )
        total = jnp.sum(jnp.where(mine, weights, 0.0), axis=1, keepdims=True)
        gate[...] = jnp.broadcast_to(total, (count, HD))

    return call(
        body,
        (shape((count, tokens)), shape((count, HD), F32)),
        2 * chips,
        [pltpu.VMEM((tokens, HD), F32)],
        flops=100_000_000,
    )(scalars, *own, *partner)


def stream(body, operands, held, later, out, scratch):
    total = len(operands)
    experts, depth, width = held.shape

    def kernel(*refs):
        w_ref = refs[total]
        if later is None:
            body(refs[:total], refs[total + 1], refs[total + 2 :], w_ref)
            return
        copies = pieces_of(refs[total + 1], later[1], refs[total + 3], refs[-1])
        for copy in copies:
            copy.start()
        body(refs[:total], refs[total + 2], refs[total + 4 : -1], w_ref)
        for copy in copies:
            copy.wait()

    vmem = pl.BlockSpec(memory_space=pltpu.VMEM)
    extra = later is not None
    return pl.pallas_call(
        kernel,
        out_shape=(out,) + ((pltpu.VMEM((experts,) + later[0].shape[1:], BF16),) if extra else ()),
        in_specs=[vmem] * (total + 1) + [pl.BlockSpec(memory_space=pltpu.HBM)] * extra,
        out_specs=(vmem,) * (1 + extra),
        scratch_shapes=list(scratch) + [pltpu.SemaphoreType.DMA((experts, PIECES))] * extra,
        compiler_params=pltpu.CompilerParams(vmem_limit_bytes=6 << 20),
        cost_estimate=pl.CostEstimate(
            flops=2 * out.shape[0] * depth * width,
            transcendentals=0,
            bytes_accessed=2 * experts * depth * width,
        ),
    )(*operands, held, *((in_hbm(later[0]),) if extra else ()))


def expert_in(chips, own, partner, pick, held, later, first, slots):
    rows, depth = own[0].shape
    tokens = 2 * chips * rows
    experts, _, width = held.shape

    def body(refs, out, scratch, w_ref):
        table, picked = scratch
        for k in range(chips):
            for t in range(2):
                b = 2 * k + t
                table[b * rows : (b + 1) * rows] = refs[t * chips + k][...]
        at = slice(first * slots, (first + experts) * slots)
        picked[...] = dot(refs[-1][at], table[...]).astype(BF16)
        for e in range(experts):
            at = slice(e * slots, (e + 1) * slots)
            out[at] = dot(picked[at], w_ref[e]).astype(BF16)

    return stream(
        body, (*own, *partner, pick), held, later, shape((experts * slots, width)),
        [pltpu.VMEM((tokens, depth), BF16), pltpu.VMEM((experts * slots, depth), BF16)],
    )


def expert_out(before, before_other, gate, held, later, first, slots):
    experts, _, width = held.shape

    def body(refs, out, scratch, w_ref):
        a_ref, b_ref, g_ref = refs
        for e in range(experts):
            at = slice(e * slots, (e + 1) * slots)
            total = a_ref[at].astype(F32) + b_ref[at].astype(F32)
            gates = g_ref[(first + e) * slots : (first + e + 1) * slots, :1]
            hidden = total / (1.0 + jnp.exp(-total)) * gates
            out[at] = dot(hidden.astype(BF16), w_ref[e]).astype(BF16)

    return stream(body, (before, before_other, gate), held, later, shape((experts * slots, width)), [])


def combine(chips, pick, produced, tile=512):
    count, tokens = pick.shape
    chunks = len(produced)
    step, cols = produced[0].shape
    rows = tokens // (2 * chips)

    def body(p_ref, *refs):
        mine, theirs = refs[chunks:]
        total = None
        for n in range(chunks):
            part = dot(p_ref[n * step : (n + 1) * step], refs[n][...], ((0,), (0,)))
            total = part if total is None else total + part
        for k in range(chips):
            at = 2 * k * rows
            mine[k] = total[at : at + rows]
            theirs[k] = total[at + rows : at + 2 * rows].astype(BF16)

    return pl.pallas_call(
        body,
        grid=(cols // tile,),
        out_shape=(shape((chips, rows, cols), F32), shape((chips, rows, cols))),
        in_specs=[pl.BlockSpec((count, tokens), lambda n: (0, 0))]
        + [pl.BlockSpec((step, tile), lambda n: (0, n))] * chunks,
        out_specs=(pl.BlockSpec((chips, rows, tile), lambda n: (0, 0, n)),) * 2,
        compiler_params=pltpu.CompilerParams(vmem_limit_bytes=10 << 20),
        cost_estimate=pl.CostEstimate(
            flops=2 * count * tokens * cols, transcendentals=0, bytes_accessed=4 * count * cols
        ),
    )(pick, *produced)


def device_by_chips(
    chips,
    queries,
    cache_keys,
    cache_values,
    tree_keys,
    tree_values,
    parents,
    lengths,
    out_weight,
    in_experts,
    out_experts,
    gate_experts,
    gate_weights,
):
    count = 2 * chips
    index = lax.axis_index("seq")
    chip, core = index >> 1, index & 1
    local = in_experts.shape[0]
    top = gate_experts.shape[1]
    slots = count * CAP
    cached, tree = cache_keys.shape[1], tree_keys.shape[1]
    scalars = jnp.stack(
        [chip, core, lengths[0], lax.axis_index("req"), index * local]
    ).astype(jnp.int32)

    def to_partner(a):
        return lax.ppermute(a, "seq", [(i, i ^ 1) for i in range(count)])

    def to_chip(a, k):
        return lax.ppermute(a, "seq", [(i, i ^ (2 * k)) for i in range(count)])

    def over_req(a):
        return lax.ppermute(a, "req", [(0, 1), (1, 0)])

    def scatter_sum(mine, theirs):
        paired = mine + to_partner(theirs).astype(F32)
        sent = [to_chip(paired[k].astype(BF16), k) for k in range(1, chips)]
        total = paired[0]
        for piece in sent:
            total = total + piece.astype(F32)
        return total.astype(BF16)

    packed = pack_blocks(
        scalars, chips, queries[0].transpose(1, 0, 2), cache_keys[0], tree_keys[0], cache_values[0], tree_values[0],
        gate_experts.T, gate_weights.T,
    )
    own = [packed[0]] + [to_chip(packed[k], k) for k in range(1, chips)]
    partner = [to_partner(block) for block in own]
    step = max(1, local // CHUNKS)
    held = fetch(out_weight, 0, chips)
    held_in, held_out = [None] * (local // step), []
    for n in range(local // step):
        held_in[n] = fetch(in_experts, n * step, step)
    bias = visibility(scalars, chips, cached, tree, parents)
    first_row = packed[0].shape[0] - gate_experts.shape[0]
    pick, gate = routing(scalars, chips, own, partner, local, slots, top, first_row)
    far = range(chips // 2, chips)
    results = attend(scalars, chips, cached, tree, own, partner, bias, far)
    results = [to_chip(part, k) for k, part in zip(far, results, strict=True)]
    near = attend(scalars, chips, cached, tree, own, partner, bias, range(chips // 2))
    near = [near[0]] + [to_chip(near[k], k) for k in range(1, chips // 2)]
    results = near + results
    swapped = [over_req(block) for block in results]
    here = project(scalars, chips, 0, results, held)
    attended = scatter_sum(*project(scalars, chips, 1, swapped, held, here))
    rows = [attended] + [to_chip(attended, k) for k in range(1, chips)]
    rows_partner = [to_partner(block) for block in rows]
    chunks = local // step
    late = chunks // 2
    before, produced = [], []
    for n in range(chunks):
        later = (out_experts, (n - late) * step) if n >= late else None
        part, *fetched = expert_in(chips, rows, rows_partner, pick, held_in[n], later, n * step, slots)
        before.append(part)
        held_out += fetched
    before_other = [over_req(part) for part in before]
    for n in range(chunks):
        later = (out_experts, (chunks - late + n) * step) if n < late else None
        part, *fetched = expert_out(before[n], before_other[n], gate, held_out[n], later, n * step, slots)
        produced.append(part)
        held_out += fetched
    return (attended, scatter_sum(*combine(chips, pick, produced)))


def ancestors(parent_row, node_count):
    node_ids = jnp.arange(node_count, dtype=jnp.int32)
    parent_hit = (node_ids[None, :] == parent_row[:, None]).astype(jnp.float32)
    reached = jnp.maximum(parent_hit, jnp.eye(node_count, dtype=jnp.float32))
    for _ in range(max(1, (node_count - 1).bit_length())):
        reached = jnp.minimum(jnp.dot(reached, reached, precision=lax.Precision.HIGHEST), 1.0)
    return reached


def per_device(
    queries,
    cache_keys,
    cache_values,
    tree_keys,
    tree_values,
    parents,
    lengths,
    out_weight,
    in_experts,
    out_experts,
    gate_experts,
    gate_weights,
):
    seq_index = lax.axis_index("seq")
    ctx_local = cache_keys.shape[1]
    nodes_local = queries.shape[1]
    kv_local = queries.shape[2]
    gathered = lax.all_gather(queries, "seq", axis=1, tiled=True)
    node_count = gathered.shape[1]
    reached = ancestors(parents[0], node_count)
    tree_seen = lax.dynamic_slice_in_dim(reached, seq_index * nodes_local, nodes_local, 1) > 0.5
    positions = seq_index * ctx_local + jnp.arange(ctx_local, dtype=jnp.int32)
    context_seen = jnp.broadcast_to((positions < lengths[0])[None, :], (node_count, ctx_local))
    visible = jnp.concatenate([context_seen, tree_seen], axis=1)[None]
    factor = 1.0 / math.sqrt(HD)
    outputs, maxima, totals = ([], [], [])
    for head_pair in range(kv_local):
        first_col = head_pair * HD
        key_rows = jnp.concatenate(
            [
                cache_keys[0, :, first_col : first_col + HD],
                tree_keys[0, :, first_col : first_col + HD],
            ],
            axis=0,
        )
        value_rows = jnp.concatenate(
            [
                cache_values[0, :, first_col : first_col + HD],
                tree_values[0, :, first_col : first_col + HD],
            ],
            axis=0,
        )
        query_block = gathered[0, :, head_pair].reshape(node_count, GROUP, HD)
        scores = (
            jnp.einsum("ngd,kd->gnk", query_block, key_rows, preferred_element_type=jnp.float32)
            * factor
        )
        masked = jnp.where(visible, scores, NEG_FILL)
        row_max = jnp.max(masked, axis=-1)
        weights = jnp.where(visible, jnp.exp(masked - row_max[..., None]), 0.0)
        weights_low = weights.astype(jnp.bfloat16)
        outputs.append(
            jnp.einsum("gnk,kd->gnd", weights_low, value_rows, preferred_element_type=jnp.float32)
        )
        maxima.append(row_max)
        totals.append(jnp.sum(weights, axis=-1))
    partial_out = jnp.stack(outputs)
    partial_max = jnp.stack(maxima)
    partial_sum = jnp.stack(totals)
    pieces = (
        lax.all_to_all(partial_out[None], "seq", split_axis=2, concat_axis=0, tiled=True),
        lax.all_to_all(partial_max[None], "seq", split_axis=2, concat_axis=0, tiled=True),
        lax.all_to_all(partial_sum[None], "seq", split_axis=2, concat_axis=0, tiled=True),
    )
    larger = jnp.max(pieces[1], axis=0)
    scales = jnp.exp(pieces[1] - larger[None])
    merged = jnp.sum(pieces[0] * scales[..., None], axis=0)
    summed = jnp.sum(pieces[2] * scales, axis=0)
    attention = merged / summed[..., None]
    attention = jnp.transpose(attention, (2, 0, 1, 3)).reshape(node_count, -1).astype(jnp.bfloat16)
    head_rows = lax.all_gather(attention, "req", axis=0, tiled=True)
    projector = out_weight.reshape(-1, out_weight.shape[2])
    attended = lax.psum_scatter(
        jnp.dot(head_rows, projector, preferred_element_type=jnp.float32),
        ("seq", "side"),
        scatter_dimension=0,
        tiled=True,
    ).astype(jnp.bfloat16)
    local_experts = in_experts.shape[0]
    flat_ids = gate_experts.reshape(-1)
    expert_hit = (flat_ids[:, None] == jnp.arange(EXPERTS, dtype=jnp.int32)[None, :]).astype(
        jnp.int32
    )
    earlier = jnp.cumsum(expert_hit, axis=0) - expert_hit
    slot_rank = jnp.sum(earlier * expert_hit, axis=1)
    slot_ids = (flat_ids * CAP + slot_rank).reshape(gate_experts.shape)
    slot_count = EXPERTS * CAP
    matches = jnp.arange(slot_count, dtype=jnp.int32)[:, None, None] == slot_ids[None]
    placing = jnp.any(matches, axis=2).astype(jnp.bfloat16)
    mixing = jnp.sum(jnp.where(matches, gate_weights[None], 0.0), axis=2)
    outgoing = jnp.dot(placing, attended, preferred_element_type=jnp.float32).astype(jnp.bfloat16)
    device_count = EXPERTS // local_experts
    outgoing = outgoing.reshape(device_count, local_experts, CAP, -1)
    before = jnp.einsum(
        "sekd,edf->sekf",
        lax.all_to_all(outgoing, ("seq", "side"), split_axis=0, concat_axis=0, tiled=True),
        in_experts,
        preferred_element_type=jnp.float32,
    )
    hidden_sum = lax.psum(before, "req")
    hidden = jax.nn.silu(hidden_sum).astype(jnp.bfloat16)
    produced = jnp.einsum(
        "sekf,efd->sekd", hidden, out_experts, preferred_element_type=jnp.float32
    ).astype(jnp.bfloat16)
    came_back = lax.all_to_all(produced, ("seq", "side"), split_axis=0, concat_axis=0, tiled=True)
    slot_rows = came_back.reshape(slot_count, -1).astype(jnp.float32)
    expert_mix = jnp.dot(mixing.T, slot_rows, precision=lax.Precision.HIGHEST)
    return (attended, expert_mix.astype(jnp.bfloat16))


def solution(mesh):
    sizes = dict(mesh.shape)
    chips = sizes["seq"] // 2
    by_chips = (
        sizes["side"] == 1 and sizes["req"] == 2 and chips * (chips - 1) > 0 and chips & (chips - 1) == 0
    )

    def run(*operands):
        if by_chips and operands[0].shape[2] == chips:
            return device_by_chips(chips, *operands)
        return per_device(*operands)

    placed = (
        P(("groups", "req"), "seq", "side", None),
        P(("groups", "req"), "seq", "side"),
        P(("groups", "req"), "seq", "side"),
        P(("groups", "req"), "seq", "side"),
        P(("groups", "req"), "seq", "side"),
        P(("groups", "req"), None),
        P(("groups", "req")),
        P("side", "seq", "req"),
        P(("seq", "side"), "req", None),
        P(("seq", "side"), None, "req"),
        P(("groups", "seq", "side"), None),
        P(("groups", "seq", "side"), None),
    )
    return jax.shard_map(
        run,
        mesh=mesh,
        in_specs=placed,
        out_specs=(P(("groups", "seq", "side"), "req"), P(("groups", "seq", "side"), "req")),
        check_vma=False,
    )
```
